32 devices in a mesh: batch: 8 (over y, x, core), head: 4 (over z).
Axes of the slice: x: 2, y: 2, z: 4, core: 2. Of those that a mesh axis runs over, the one named last changes fastest.
Arguments:
- inputs: bfloat16 [8, 128, 2048], P(None, 'batch', 'head'), parts along dimension 1, may hold values from -6 to 6
- in_weight: bfloat16 [2048, 4, 384], P(None, 'head'), may hold values from -0.125 to 0.125
- gate_weight: bfloat16 [2048, 4], P(None, 'head'), may hold values from -0.125 to 0.125
- gate_bias: float32 [4], P('head'), may hold values from -2 to 3
- norm_gain: float32 [512], P('head'), may hold values from 0.1 to 1.9
- out_weight: bfloat16 [512, 2048], P('head'), may hold values from -0.375 to 0.375
- inv_gram: float32 [128, 4, 128, 128], P('batch', 'head'), parts along dimension 0, may hold values from -17 to 17, as said below
- value_key: float32 [128, 4, 128, 128], P('batch', 'head'), parts along dimension 0, may hold values from -6 to 6
Outputs:
- layer_out: float32 [8, 128, 2048], P(None, 'batch', 'head'), parts along dimension 1
The draws below stay inside these ranges and needn't reach their ends.
There are 8 independent parts, one for each index of `batch`. The reference program is written for one: setup_inputs(seed, part) draws one part's arguments, and reference() takes and returns one part's arrays. A program takes and returns all parts, laid end to end along the dimension named above; an argument that names none is the same for every part. Nothing has to cross between parts.
Inputs may be any that keep to these rules, and one draw needn't show every extreme that they name: `inv_gram`: each [128, 128] matrix is symmetric positive definite.
All inputs are finite; a program needn't handle non-finite values.
Results may differ from the reference program's by a relative error of at most 0.0029.
Values may be sent and summed in bfloat16 or wider, within the bound.
No kernel may reach another device: no remote copies, remote signals or barrier semaphores. Data moves between devices by JAX's collectives and lax.ppermute only.
A program may use at most 64 MiB of HBM per device.

```python
import jax
import jax.numpy as jnp
from jax import lax

D = 2048
DH = 128
SEQS = 16
STEPS = 8
HEADS = 4


def draw_inv_gram(key, part):
    shape = (SEQS, HEADS, DH, DH)
    entries = jnp.clip(jax.random.normal(key, shape, jnp.float32), -4.0, 4.0)
    gram_part = jnp.einsum('shij,shkj->shik', entries, entries, precision=lax.Precision.HIGHEST) / DH
    return 0.5 * jnp.eye(DH, dtype=jnp.float32) + gram_part


def draw_value_key(key, part):
    shape = (SEQS, HEADS, DH, DH)
    rising = 3.0 ** (jnp.arange(HEADS, dtype=jnp.float32) / max(HEADS - 1, 1))
    entries = jnp.clip(jax.random.normal(key, shape, jnp.float32), -4.0, 4.0)
    scales = 0.12 * jnp.broadcast_to(rising[None, :], (SEQS, HEADS))
    return entries * scales[:, :, None, None]


def raised(values, key, source, target, blocks, factor):
    owner, partner = [(jnp.arange(values.shape[dim]) // (values.shape[dim] // blocks)).reshape([-1 if axis == dim else 1 for axis in range(values.ndim)]) for dim in (source, target)]
    chosen = jax.random.permutation(key, blocks)[partner]
    strong = (owner == chosen) | (owner == (partner + blocks // 2) % blocks)
    return jnp.where(strong, factor * values, values)


def steps_of(rng, shape, split, low, high):
    loudness = 1.0
    for dim, shards_of in split:
        draws = jax.random.uniform(jax.random.fold_in(jax.random.fold_in(rng, 6), dim), (shards_of,), jnp.float32, low / len(split), high / len(split))
        loudness = loudness * jnp.repeat(jnp.exp(draws), shape[dim] // shards_of).reshape((-1,) + (1,) * (len(shape) - 1 - dim))
    return loudness


def normal_values(own_key, extent, spread, reach, cuts=(), kind=jnp.bfloat16):
    loudness = steps_of(own_key, extent, cuts, -0.22, 0.18) if cuts else 1.0
    array = jax.random.normal(own_key, extent, jnp.float32) * spread * loudness
    return jnp.minimum(jnp.maximum(array, -reach), reach).astype(kind)


def heavy_noise(rng, dims, width, reach, shards, heavy, kind=jnp.bfloat16):
    values = width * jax.random.normal(rng, dims, jnp.float32)
    if shards:
        values = values * steps_of(rng, dims, shards, -0.22, 0.18)
    return jnp.clip(raised(values, jax.random.fold_in(rng, 3), *heavy), -reach, reach).astype(kind)


def setup_inputs(seed: int = 0, part: int = 0) -> dict:
    splits = jax.random.split(jax.random.key(seed), 9)
    part_splits = jax.random.split(jax.random.fold_in(splits[8], part), 9)
    inputs = normal_values(part_splits[0], (STEPS, SEQS, D), 1.0, 6.0, ((2, 4),))
    in_weight = normal_values(splits[1], (D, HEADS, 3 * DH), D ** -0.5, 0.125, ((1, 4),))
    gate_weight = normal_values(splits[2], (D, HEADS), D ** -0.5, 0.125, ((1, 4),))
    gate_bias = jnp.clip(-2.0 + 5.0 * jax.random.uniform(splits[3], (HEADS,), jnp.float32) ** steps_of(splits[3], (HEADS,), ((0, 4),), -0.2, 0.2), -2.0, 3.0)
    norm_gain = jnp.clip(1.0 + 0.18 * jax.random.normal(splits[4], (HEADS * DH,), jnp.float32), 0.1, 1.9)
    out_weight = heavy_noise(splits[5], (HEADS * DH, D), (HEADS * DH) ** -0.5, 0.375, ((0, 4),), (0, 1, 4, 2.0))
    inv_gram = draw_inv_gram(jax.random.fold_in(jax.random.fold_in(splits[8], part), 71), part)
    value_key = draw_value_key(jax.random.fold_in(jax.random.fold_in(splits[8], part), 71), part)
    return dict(inputs=inputs, in_weight=in_weight, gate_weight=gate_weight, gate_bias=gate_bias, norm_gain=norm_gain, out_weight=out_weight, inv_gram=inv_gram, value_key=value_key)


def advance(gram_inv, memory, projected, gate, gate_bias, head_size):
    batch_rows, local_heads = gate.shape
    pieces = projected.reshape(batch_rows, local_heads, 3 * head_size)
    queries = pieces[..., :head_size]
    keys_now = pieces[..., head_size:2 * head_size]
    values_now = pieces[..., 2 * head_size:]
    forget = 0.8 + 0.2 * jax.nn.sigmoid(gate + gate_bias)
    keys_now = keys_now * lax.rsqrt(lax.optimization_barrier(jnp.sum(keys_now * keys_now, axis=-1, keepdims=True)) + 1e-06)
    queries = queries * lax.rsqrt(lax.optimization_barrier(jnp.sum(queries * queries, axis=-1, keepdims=True)) + 1e-06)
    gram_key = jnp.einsum('bhij,bhj->bhi', gram_inv, keys_now, precision=lax.Precision.HIGHEST)
    denominator = forget + lax.optimization_barrier(jnp.sum(keys_now * gram_key, axis=-1))
    gram_inv = (gram_inv - gram_key[..., :, None] * gram_key[..., None, :] / denominator[..., None, None]) / forget[..., None, None]
    memory = forget[..., None, None] * memory + values_now[..., :, None] * keys_now[..., None, :]
    gram_query = jnp.einsum('bhij,bhj->bhi', gram_inv, queries, precision=lax.Precision.HIGHEST)
    readout = jnp.einsum('bhij,bhj->bhi', memory, gram_query, precision=lax.Precision.HIGHEST)
    return (gram_inv, memory, readout.reshape(batch_rows, local_heads * head_size))

def reference(inputs, in_weight, gate_weight, gate_bias, norm_gain, out_weight, inv_gram, value_key):
    weight_flat = in_weight.reshape(D, HEADS * 3 * DH)
    gram_inv = inv_gram
    memory = value_key
    results = []
    for position in range(STEPS):
        projected = jnp.dot(inputs[position], weight_flat, preferred_element_type=jnp.float32)
        gate = jnp.dot(inputs[position], gate_weight, preferred_element_type=jnp.float32)
        gram_inv, memory, readout = advance(gram_inv, memory, projected, gate, gate_bias, DH)
        mean_square = lax.optimization_barrier(jnp.mean(readout * readout, axis=-1))
        hidden = (norm_gain * readout * lax.rsqrt(mean_square + 1e-06)[:, None]).astype(jnp.bfloat16)
        results.append(jnp.dot(hidden, out_weight, preferred_element_type=jnp.float32))
    return jnp.stack(results, axis=0)
```

```python
import functools

import jax
import jax.numpy as jnp
from jax import lax
from jax.experimental import pallas as pl
from jax.experimental.pallas import tpu as pltpu
from jax.sharding import PartitionSpec as P


EPS = 1e-06


def dot(a, b, dims=((1,), (0,))):
    return lax.dot_general(a, b, (dims, ((), ())), preferred_element_type=jnp.float32)


def lane_sum(a):
    return jnp.sum(a, axis=-1, keepdims=True)


def split(a):
    high = a.astype(jnp.bfloat16)
    return high, (a - high.astype(jnp.float32)).astype(jnp.bfloat16)


def partner(index, shift, size):
    return index ^ shift if size & (size - 1) == 0 else (index + shift) % size


def source(index, shift, size):
    return index ^ shift if size & (size - 1) == 0 else (index - shift) % size


def send(array, shift, size):
    return lax.ppermute(array, "head", [(i, partner(i, shift, size)) for i in range(size)])


def pack_kernel(gram_ref, memory_ref, gram_out, memory_out):
    pairs, width, _ = gram_out.shape
    size = width // 2
    for p in range(pairs):
        for i in range(2):
            high, low = split(gram_ref[2 * p + i])
            gram_out[p, :size, i * size : (i + 1) * size] = high
            gram_out[p, size:, i * size : (i + 1) * size] = low
            high, low = split(memory_ref[2 * p + i])
            memory_out[p, i * size : (i + 1) * size, :size] = high
            memory_out[p, i * size : (i + 1) * size, size:] = low


def mesa_kernel(shards, steps, *refs):
    x_refs = refs[:shards]
    w_ref, gate_ref, bias_ref, gain_ref, gram_ref, memory_ref, out_ref, kq, ab, xs, ys = refs[shards:]
    rows, features = x_refs[0].shape
    seqs = rows // steps
    size = out_ref.shape[1]
    me = lax.axis_index("head")
    projected = 0.0
    gate = 0.0
    for s in range(shards):
        off = pl.multiple_of(source(me, s, shards) * features, features)
        projected = projected + dot(x_refs[s][...], w_ref[pl.ds(off, features), :])
        gate = gate + dot(x_refs[s][...], gate_ref[pl.ds(off, features), :])
    forget = 0.8 + 0.2 * jax.nn.sigmoid(gate + bias_ref[0, 0])
    queries = projected[:, :size]
    keys = projected[:, size : 2 * size]
    values = projected[:, 2 * size :]
    keys = keys * lax.rsqrt(lane_sum(keys * keys) + EPS)
    queries = queries * lax.rsqrt(lane_sum(queries * queries) + EPS)
    kq[:rows] = keys
    kq[rows:] = queries
    for p in range(seqs // 2):
        parts = []
        for i in range(2):
            parts += split(kq[pl.ds(2 * p + i, 2 * steps, stride=seqs), :])
        lhs = jnp.concatenate(parts, axis=0)
        res = dot(jnp.concatenate([lhs, lhs], axis=1), gram_ref[p])
        for i in range(2):
            half = res[i * 4 * steps : (i + 1) * 4 * steps, i * size : (i + 1) * size]
            ab[pl.ds(2 * p + i, 2 * steps, stride=seqs), :] = half[: 2 * steps] + half[2 * steps :]

    def at(array, t):
        return array[t * seqs : (t + 1) * seqs]

    k = [at(keys, t) for t in range(steps)]
    q = [at(queries, t) for t in range(steps)]
    a = [ab[t * seqs : (t + 1) * seqs, :] for t in range(steps)]
    b = [ab[rows + t * seqs : rows + (t + 1) * seqs, :] for t in range(steps)]
    decay = []
    for t in range(steps):
        decay.append(at(forget, t) if t == 0 else decay[-1] * at(forget, t))
    for s in range(steps):
        g = a[s]
        u = g / (decay[s] + lane_sum(g * k[s]))
        for t in range(s + 1, steps):
            a[t] = a[t] - u * lane_sum(g * k[t])
        for t in range(s, steps):
            b[t] = b[t] - u * lane_sum(g * q[t])
    for t in range(steps):
        xs[t * seqs : (t + 1) * seqs, :] = b[t]
    for p in range(seqs // 2):
        parts = []
        for i in range(2):
            parts += split(xs[pl.ds(2 * p + i, steps, stride=seqs), :])
        lhs = jnp.concatenate(parts, axis=0)
        res = dot(jnp.concatenate([lhs, lhs], axis=1), memory_ref[p], ((1,), (1,)))
        for i in range(2):
            half = res[i * 2 * steps : (i + 1) * 2 * steps, i * size : (i + 1) * size]
            ys[pl.ds(2 * p + i, steps, stride=seqs), :] = half[:steps] + half[steps:]
    scaled = [at(values, t) / decay[t] for t in range(steps)]
    for t in range(steps):
        y = ys[t * seqs : (t + 1) * seqs, :]
        for s in range(t + 1):
            y = y + scaled[s] * lane_sum(k[s] * b[t])
        out_ref[t * seqs : (t + 1) * seqs, :] = y
    out_ref[rows:, :] = jnp.broadcast_to(gain_ref[...], (out_ref.shape[0] - rows, size))


def output_kernel(shards, *refs):
    r_refs = refs[:shards]
    w_refs = refs[shards : 2 * shards]
    out_ref = refs[2 * shards]
    rows = out_ref.shape[0]
    size = r_refs[0].shape[1]
    total = 0.0
    for s in range(shards):
        r = r_refs[s][:rows]
        total = total + lane_sum(r * r)
    scale = lax.rsqrt(total / (size * shards) + EPS)
    acc = 0.0
    for s in range(shards):
        hidden = (r_refs[s][rows : rows + 1] * r_refs[s][:rows] * scale).astype(jnp.bfloat16)
        acc = acc + dot(hidden, w_refs[s][...])
    out_ref[...] = acc


def local(inputs, in_weight, gate_weight, gate_bias, norm_gain, out_weight, inv_gram, value_key):
    steps, seqs, features = inputs.shape
    d_model, local_heads, width = in_weight.shape
    assert local_heads == 1 and seqs % 2 == 0
    size = width // 3
    rows = steps * seqs
    shards = lax.axis_size("head")
    me = lax.axis_index("head")
    out_cols = out_weight.shape[1] // shards
    x = inputs.reshape(rows, features)
    xs = [x] + [send(x, s, shards) for s in range(1, shards)]
    ws = [lax.dynamic_slice_in_dim(out_weight, partner(me, s, shards) * out_cols, out_cols, 1) for s in range(shards)]
    ws = [ws[0]] + [send(ws[s], s, shards) for s in range(1, shards)]
    weight = in_weight.reshape(d_model, width)
    gate = jnp.broadcast_to(gate_weight.reshape(d_model, 1), (d_model, size))
    tiles = jax.ShapeDtypeStruct((seqs // 2, 2 * size, 2 * size), jnp.bfloat16)
    gram, memory = pl.pallas_call(pack_kernel, out_shape=(tiles, tiles), name="pack")(
        inv_gram.reshape(seqs, size, size), value_key.reshape(seqs, size, size)
    )
    readout = pl.pallas_call(
        functools.partial(mesa_kernel, shards, steps),
        out_shape=jax.ShapeDtypeStruct((rows + 8, size), jnp.float32),
        in_specs=[pl.BlockSpec(memory_space=pltpu.VMEM)] * (shards + 2)
        + [pl.BlockSpec(memory_space=pltpu.SMEM)]
        + [pl.BlockSpec(memory_space=pltpu.VMEM)] * 3,
        scratch_shapes=[
            pltpu.VMEM((2 * rows, size), jnp.float32),
            pltpu.VMEM((2 * rows, size), jnp.float32),
            pltpu.VMEM((rows, size), jnp.float32),
            pltpu.VMEM((rows, size), jnp.float32),
        ],
        name="mesa",
    )(*xs, weight, gate, gate_bias.reshape(1, 1), norm_gain.reshape(1, size), gram, memory)
    rs = [readout] + [send(readout, s, shards) for s in range(1, shards)]
    out = pl.pallas_call(
        functools.partial(output_kernel, shards),
        out_shape=jax.ShapeDtypeStruct((rows, out_cols), jnp.float32),
        name="output",
    )(*rs, *ws)
    return out.reshape(steps, seqs, out_cols)


def solution(mesh):
    in_specs = (
        P(None, "batch", "head"),
        P(None, "head", None),
        P(None, "head"),
        P("head"),
        P("head"),
        P("head", None),
        P("batch", "head", None, None),
        P("batch", "head", None, None),
    )
    out_specs = P(None, "batch", "head")
    return jax.shard_map(local, mesh=mesh, in_specs=in_specs, out_specs=out_specs, check_vma=False)
```

```python
import functools

import jax
import jax.numpy as jnp
from jax import lax
from jax.experimental import pallas as pl
from jax.experimental.pallas import tpu as pltpu
from jax.sharding import PartitionSpec as P


EPS = 1e-06
VMEM_BYTES = 16 * 2**20


def dot(a, b, dims=((1,), (0,))):
    return lax.dot_general(a, b, (dims, ((), ())), preferred_element_type=jnp.float32)


def lane_sum(a):
    return jnp.sum(a, axis=-1, keepdims=True)


def split(a):
    high = a.astype(jnp.bfloat16)
    return high, (a - high.astype(jnp.float32)).astype(jnp.bfloat16)


def partner(index, shift, size):
    return index ^ shift if size & (size - 1) == 0 else (index + shift) % size


def source(index, shift, size):
    return index ^ shift if size & (size - 1) == 0 else (index - shift) % size


def send(array, shift, size):
    return lax.ppermute(array, "head", [(i, partner(i, shift, size)) for i in range(size)])


def call(kernel, name, out_shape, scratch=()):
    return pl.pallas_call(
        kernel,
        out_shape=out_shape,
        scratch_shapes=[pltpu.VMEM(shape, dtype) for shape, dtype in scratch],
        name=name,
        compiler_params=pltpu.CompilerParams(vmem_limit_bytes=VMEM_BYTES),
    )


def pack_kernel(gram_ref, memory_ref, gram_out, memory_out):
    pairs, width, _ = gram_out.shape
    size = width // 2
    for p in range(pairs):
        for i in range(2):
            high, low = split(gram_ref[2 * p + i])
            gram_out[p, :size, i * size : (i + 1) * size] = high
            gram_out[p, size:, i * size : (i + 1) * size] = low
            high, low = split(memory_ref[2 * p + i])
            memory_out[p, i * size : (i + 1) * size, :size] = high
            memory_out[p, i * size : (i + 1) * size, size:] = low


def slice_kernel(shards, weight_ref, own_ref, *piece_refs):
    me = lax.axis_index("head")
    half, cols = piece_refs[0].shape
    mine = pl.multiple_of((lax.axis_index("batch") % 2) * half, half)
    own_ref[...] = weight_ref[:, pl.ds(pl.multiple_of(me * cols, cols), cols)]
    for s in range(1, shards):
        off = pl.multiple_of(partner(me, s, shards) * cols, cols)
        piece_refs[s - 1][...] = weight_ref[pl.ds(mine, half), pl.ds(off, cols)]


def join_kernel(*refs):
    half = refs[0].shape[0]
    for s, ref in enumerate(refs[:-1]):
        refs[-1][s * half : (s + 1) * half] = ref[...]


def mesa_kernel(shards, steps, *refs):
    x_refs = refs[:shards]
    w_ref, gate_ref, bias_ref, gain_ref, gram_ref, memory_ref, out_ref, kq, ab, xs, ys = refs[shards:]
    rows, features = x_refs[0].shape
    seqs = rows // steps
    size = out_ref.shape[1]
    me = lax.axis_index("head")
    projected = 0.0
    gate = 0.0
    for s in range(shards):
        off = pl.multiple_of(source(me, s, shards) * features, features)
        projected = projected + dot(x_refs[s][...], w_ref[pl.ds(off, features), :])
        gate_rows = jnp.broadcast_to(gate_ref[:, pl.ds(off, features)], (size, features))
        gate = gate + dot(x_refs[s][...], gate_rows, ((1,), (1,)))
    forget = 0.8 + 0.2 * jax.nn.sigmoid(gate + bias_ref[...])
    queries = projected[:, :size]
    keys = projected[:, size : 2 * size]
    values = projected[:, 2 * size :]
    keys = keys * lax.rsqrt(lane_sum(keys * keys) + EPS)
    queries = queries * lax.rsqrt(lane_sum(queries * queries) + EPS)
    kq[:rows] = keys
    kq[rows:] = queries
    for p in range(seqs // 2):
        parts = []
        for i in range(2):
            parts += split(kq[pl.ds(2 * p + i, 2 * steps, stride=seqs), :])
        lhs = jnp.concatenate(parts, axis=0)
        res = dot(jnp.concatenate([lhs, lhs], axis=1), gram_ref[p])
        for i in range(2):
            half = res[i * 4 * steps : (i + 1) * 4 * steps, i * size : (i + 1) * size]
            ab[pl.ds(2 * p + i, 2 * steps, stride=seqs), :] = half[: 2 * steps] + half[2 * steps :]

    def at(array, t):
        return array[t * seqs : (t + 1) * seqs]

    k = [at(keys, t) for t in range(steps)]
    q = [at(queries, t) for t in range(steps)]
    a = [ab[t * seqs : (t + 1) * seqs, :] for t in range(steps)]
    b = [ab[rows + t * seqs : rows + (t + 1) * seqs, :] for t in range(steps)]
    decay = []
    for t in range(steps):
        decay.append(at(forget, t) if t == 0 else decay[-1] * at(forget, t))
    for s in range(steps):
        g = a[s]
        u = g / (decay[s] + lane_sum(g * k[s]))
        for t in range(s + 1, steps):
            a[t] = a[t] - u * lane_sum(g * k[t])
        for t in range(s, steps):
            b[t] = b[t] - u * lane_sum(g * q[t])
    for t in range(steps):
        xs[t * seqs : (t + 1) * seqs, :] = b[t]
    for p in range(seqs // 2):
        parts = []
        for i in range(2):
            parts += split(xs[pl.ds(2 * p + i, steps, stride=seqs), :])
        lhs = jnp.concatenate(parts, axis=0)
        res = dot(jnp.concatenate([lhs, lhs], axis=1), memory_ref[p], ((1,), (1,)))
        for i in range(2):
            half = res[i * 2 * steps : (i + 1) * 2 * steps, i * size : (i + 1) * size]
            ys[pl.ds(2 * p + i, steps, stride=seqs), :] = half[:steps] + half[steps:]
    scaled = [at(values, t) / decay[t] for t in range(steps)]
    for t in range(steps):
        y = ys[t * seqs : (t + 1) * seqs, :]
        for s in range(t + 1):
            y = y + scaled[s] * lane_sum(k[s] * b[t])
        out_ref[t * seqs : (t + 1) * seqs, :] = y
    out_ref[rows:, :] = jnp.broadcast_to(gain_ref[...], (out_ref.shape[0] - rows, size))


def output_kernel(shards, *refs):
    r_refs = refs[:shards]
    own_ref = refs[shards]
    mine_ref, other_ref, out_ref, w_scr = refs[shards + 1 :]
    rows = out_ref.shape[0]
    half = mine_ref.shape[0] // (shards - 1)
    width = own_ref.shape[0]
    mine = pl.multiple_of((lax.axis_index("batch") % 2) * half, half)
    other = pl.multiple_of(half - mine, half)
    w_scr[:width] = own_ref[...]
    for s in range(1, shards):
        w_scr[pl.ds(s * width + mine, half), :] = mine_ref[(s - 1) * half : s * half]
        w_scr[pl.ds(s * width + other, half), :] = other_ref[(s - 1) * half : s * half]
    size = r_refs[0].shape[1]
    total = 0.0
    for s in range(shards):
        r = r_refs[s][:rows]
        total = total + lane_sum(r * r)
    scale = lax.rsqrt(total / (size * shards) + EPS)
    hidden = [(r[rows : rows + 1] * r[:rows] * scale).astype(jnp.bfloat16) for r in r_refs]
    out_ref[...] = dot(jnp.concatenate(hidden, axis=1), w_scr[...])


def local(inputs, in_weight, gate_weight, gate_bias, norm_gain, out_weight, inv_gram, value_key):
    steps, seqs, features = inputs.shape
    d_model, local_heads, width = in_weight.shape
    assert local_heads == 1 and seqs % 2 == 0 and lax.axis_size("batch") % 2 == 0
    size = width // 3
    rows = steps * seqs
    shards = lax.axis_size("head")
    me = lax.axis_index("head")
    out_cols = out_weight.shape[1] // shards
    x = inputs.reshape(rows, features)
    groups = lax.axis_size("batch")
    half = size // 2
    xs = [send(x, s, shards) for s in range(shards - 1, 0, -1)] + [x]
    xs.reverse()
    piece = jax.ShapeDtypeStruct((half, out_cols), jnp.bfloat16)
    w_own, *ws = call(
        functools.partial(slice_kernel, shards),
        "slice",
        [jax.ShapeDtypeStruct((size, out_cols), jnp.bfloat16)] + [piece] * (shards - 1),
    )(out_weight)
    ws = [send(ws[s - 1], s, shards) for s in range(shards - 1, 0, -1)]
    ws.reverse()
    weight = in_weight.reshape(d_model, width)
    tiles = jax.ShapeDtypeStruct((seqs // 2, 2 * size, 2 * size), jnp.bfloat16)
    gram, memory = call(pack_kernel, "pack", (tiles, tiles))(
        inv_gram.reshape(seqs, size, size), value_key.reshape(seqs, size, size)
    )
    readout = call(
        functools.partial(mesa_kernel, shards, steps),
        "mesa",
        jax.ShapeDtypeStruct((rows + 8, size), jnp.float32),
        [((2 * rows, size), jnp.float32)] * 2 + [((rows, size), jnp.float32)] * 2,
    )(*xs, weight, gate_weight.reshape(1, d_model), gate_bias.reshape(1, 1), norm_gain.reshape(1, size), gram, memory)
    readout, ws = lax.optimization_barrier((readout, ws))
    rs = [send(readout, s, shards) for s in range(shards - 1, 0, -1)] + [readout]
    rs.reverse()
    w_mine = call(join_kernel, "join", jax.ShapeDtypeStruct(((shards - 1) * half, out_cols), jnp.bfloat16))(*ws)
    w_other = lax.ppermute(w_mine, "batch", [(i, i ^ 1) for i in range(groups)])
    out = call(
        functools.partial(output_kernel, shards),
        "output",
        jax.ShapeDtypeStruct((rows, out_cols), jnp.float32),
        [((shards * size, out_cols), jnp.bfloat16)],
    )(*rs, w_own, w_mine, w_other)
    return out.reshape(steps, seqs, out_cols)


def solution(mesh):
    in_specs = (
        P(None, "batch", "head"),
        P(None, "head", None),
        P(None, "head"),
        P("head"),
        P("head"),
        P("head", None),
        P("batch", "head", None, None),
        P("batch", "head", None, None),
    )
    out_specs = P(None, "batch", "head")
    return jax.shard_map(local, mesh=mesh, in_specs=in_specs, out_specs=out_specs, check_vma=False)
```

```python
import functools

import jax
import jax.numpy as jnp
from jax import lax
from jax.experimental import pallas as pl
from jax.experimental.pallas import tpu as pltpu
from jax.sharding import PartitionSpec as P


EPS = 1e-06
VMEM_BYTES = 16 * 2**20


def dot(a, b, dims=((1,), (0,))):
    return lax.dot_general(a, b, (dims, ((), ())), preferred_element_type=jnp.float32)


def lane_sum(a):
    return jnp.sum(a, axis=-1, keepdims=True)


def split(a):
    high = a.astype(jnp.bfloat16)
    return high, (a - high.astype(jnp.float32)).astype(jnp.bfloat16)


def partner(index, shift, size):
    return index ^ shift if size & (size - 1) == 0 else (index + shift) % size


def source(index, shift, size):
    return index ^ shift if size & (size - 1) == 0 else (index - shift) % size


def shift_order(size):
    return [*range(size // 2, size), *range(1, size // 2)]


def exchange(arrays, size):
    got = {}
    for s in shift_order(size):
        got[s] = lax.ppermute(arrays[s], "head", [(i, partner(i, s, size)) for i in range(size)])
    return [got[s] for s in range(1, size)]


def call(kernel, out_shape, scratch=()):
    return pl.pallas_call(
        kernel,
        out_shape=out_shape,
        scratch_shapes=[pltpu.VMEM(shape, dtype) for shape, dtype in scratch],
        compiler_params=pltpu.CompilerParams(vmem_limit_bytes=VMEM_BYTES),
    )


def pack_kernel(gram_ref, memory_ref, gram_out, memory_out):
    pairs, width, _ = gram_out.shape
    size = width // 2
    for p in range(pairs):
        for i in range(2):
            high, low = split(gram_ref[2 * p + i])
            gram_out[p, :size, i * size : (i + 1) * size] = high
            gram_out[p, size:, i * size : (i + 1) * size] = low
            high, low = split(memory_ref[2 * p + i])
            memory_out[p, i * size : (i + 1) * size, :size] = high
            memory_out[p, i * size : (i + 1) * size, size:] = low


def slice_kernel(shards, weight_ref, own_ref, *piece_refs):
    me = lax.axis_index("head")
    half, cols = piece_refs[0].shape
    mine = pl.multiple_of((lax.axis_index("batch") % 2) * half, half)
    own_ref[...] = weight_ref[:, pl.ds(pl.multiple_of(me * cols, cols), cols)]
    for s in range(1, shards):
        off = pl.multiple_of(partner(me, s, shards) * cols, cols)
        piece_refs[s - 1][...] = weight_ref[pl.ds(mine, half), pl.ds(off, cols)]


def join_kernel(*refs):
    half = refs[0].shape[0]
    for s, ref in enumerate(refs[:-1]):
        refs[-1][s * half : (s + 1) * half] = ref[...]


def mesa_kernel(shards, steps, *refs):
    x_refs = refs[:shards]
    w_ref, gate_ref, bias_ref, gain_ref, gram_ref, memory_ref, out_ref, kq, ab, xs, ys = refs[shards:]
    rows, features = x_refs[0].shape
    seqs = rows // steps
    size = out_ref.shape[1]
    me = lax.axis_index("head")
    projected = 0.0
    gate = 0.0
    for s in range(shards):
        off = pl.multiple_of(source(me, s, shards) * features, features)
        projected = projected + dot(x_refs[s][...], w_ref[pl.ds(off, features), :])
        gate_rows = jnp.broadcast_to(gate_ref[:, pl.ds(off, features)], (size, features))
        gate = gate + dot(x_refs[s][...], gate_rows, ((1,), (1,)))
    forget = 0.8 + 0.2 * jax.nn.sigmoid(gate + bias_ref[...])
    queries = projected[:, :size]
    keys = projected[:, size : 2 * size]
    values = projected[:, 2 * size :]
    keys = keys * lax.rsqrt(lane_sum(keys * keys) + EPS)
    queries = queries * lax.rsqrt(lane_sum(queries * queries) + EPS)
    kq[:rows] = keys
    kq[rows:] = queries
    for p in range(seqs // 2):
        parts = []
        for i in range(2):
            parts += split(kq[pl.ds(2 * p + i, 2 * steps, stride=seqs), :])
        lhs = jnp.concatenate(parts, axis=0)
        res = dot(jnp.concatenate([lhs, lhs], axis=1), gram_ref[p])
        for i in range(2):
            half = res[i * 4 * steps : (i + 1) * 4 * steps, i * size : (i + 1) * size]
            ab[pl.ds(2 * p + i, 2 * steps, stride=seqs), :] = half[: 2 * steps] + half[2 * steps :]

    def at(array, t):
        return array[t * seqs : (t + 1) * seqs]

    k = [at(keys, t) for t in range(steps)]
    q = [at(queries, t) for t in range(steps)]
    a = [ab[t * seqs : (t + 1) * seqs, :] for t in range(steps)]
    b = [ab[rows + t * seqs : rows + (t + 1) * seqs, :] for t in range(steps)]
    decay = []
    for t in range(steps):
        decay.append(at(forget, t) if t == 0 else decay[-1] * at(forget, t))
    for s in range(steps):
        g = a[s]
        u = g / (decay[s] + lane_sum(g * k[s]))
        for t in range(s + 1, steps):
            a[t] = a[t] - u * lane_sum(g * k[t])
        for t in range(s, steps):
            b[t] = b[t] - u * lane_sum(g * q[t])
    for t in range(steps):
        xs[t * seqs : (t + 1) * seqs, :] = b[t]
    for p in range(seqs // 2):
        parts = []
        for i in range(2):
            parts += split(xs[pl.ds(2 * p + i, steps, stride=seqs), :])
        lhs = jnp.concatenate(parts, axis=0)
        res = dot(jnp.concatenate([lhs, lhs], axis=1), memory_ref[p], ((1,), (1,)))
        for i in range(2):
            half = res[i * 2 * steps : (i + 1) * 2 * steps, i * size : (i + 1) * size]
            ys[pl.ds(2 * p + i, steps, stride=seqs), :] = half[:steps] + half[steps:]
    scaled = [at(values, t) / decay[t] for t in range(steps)]
    for t in range(steps):
        y = ys[t * seqs : (t + 1) * seqs, :]
        for s in range(t + 1):
            y = y + scaled[s] * lane_sum(k[s] * b[t])
        out_ref[t * seqs : (t + 1) * seqs, :] = y
    out_ref[rows:, :] = jnp.broadcast_to(gain_ref[...], (out_ref.shape[0] - rows, size))


def output_kernel(shards, *refs):
    r_refs = refs[:shards]
    own_ref = refs[shards]
    mine_ref, other_ref, out_ref, w_scr = refs[shards + 1 :]
    rows = out_ref.shape[0]
    half = mine_ref.shape[0] // (shards - 1)
    width = own_ref.shape[0]
    mine = pl.multiple_of((lax.axis_index("batch") % 2) * half, half)
    other = pl.multiple_of(half - mine, half)
    w_scr[:width] = own_ref[...]
    for s in range(1, shards):
        w_scr[pl.ds(s * width + mine, half), :] = mine_ref[(s - 1) * half : s * half]
        w_scr[pl.ds(s * width + other, half), :] = other_ref[(s - 1) * half : s * half]
    size = r_refs[0].shape[1]
    total = 0.0
    for s in range(shards):
        r = r_refs[s][:rows]
        total = total + lane_sum(r * r)
    scale = lax.rsqrt(total / (size * shards) + EPS)
    hidden = [(r[rows : rows + 1] * r[:rows] * scale).astype(jnp.bfloat16) for r in r_refs]
    out_ref[...] = dot(jnp.concatenate(hidden, axis=1), w_scr[...])


def local(inputs, in_weight, gate_weight, gate_bias, norm_gain, out_weight, inv_gram, value_key):
    steps, seqs, features = inputs.shape
    d_model, local_heads, width = in_weight.shape
    assert local_heads == 1 and seqs % 2 == 0 and lax.axis_size("batch") % 2 == 0
    size = width // 3
    rows = steps * seqs
    shards = lax.axis_size("head")
    out_cols = out_weight.shape[1] // shards
    x = inputs.reshape(rows, features)
    groups = lax.axis_size("batch")
    half = size // 2
    xs = [x] + exchange([x] * shards, shards)
    piece = jax.ShapeDtypeStruct((half, out_cols), jnp.bfloat16)
    w_own, *ws = call(
        functools.partial(slice_kernel, shards),
        [jax.ShapeDtypeStruct((size, out_cols), jnp.bfloat16)] + [piece] * (shards - 1),
    )(out_weight)
    ws = exchange([None, *ws], shards)
    weight = in_weight.reshape(d_model, width)
    tiles = jax.ShapeDtypeStruct((seqs // 2, 2 * size, 2 * size), jnp.bfloat16)
    gram, memory = call(pack_kernel, (tiles, tiles))(
        inv_gram.reshape(seqs, size, size), value_key.reshape(seqs, size, size)
    )
    readout = call(
        functools.partial(mesa_kernel, shards, steps),
        jax.ShapeDtypeStruct((rows + 8, size), jnp.float32),
        [((2 * rows, size), jnp.float32)] * 2 + [((rows, size), jnp.float32)] * 2,
    )(*xs, weight, gate_weight.reshape(1, d_model), gate_bias.reshape(1, 1), norm_gain.reshape(1, size), gram, memory)
    rs = [readout] + exchange([readout] * shards, shards)
    w_mine = call(join_kernel, jax.ShapeDtypeStruct(((shards - 1) * half, out_cols), jnp.bfloat16))(*ws)
    w_other = lax.ppermute(w_mine, "batch", [(i, i ^ 1) for i in range(groups)])
    out = call(
        functools.partial(output_kernel, shards),
        jax.ShapeDtypeStruct((rows, out_cols), jnp.float32),
        [((shards * size, out_cols), jnp.bfloat16)],
    )(*rs, w_own, w_mine, w_other)
    return out.reshape(steps, seqs, out_cols)


def solution(mesh):
    in_specs = (
        P(None, "batch", "head"),
        P(None, "head", None),
        P(None, "head"),
        P("head"),
        P("head"),
        P("head", None),
        P("batch", "head", None, None),
        P("batch", "head", None, None),
    )
    out_specs = P(None, "batch", "head")
    return jax.shard_map(local, mesh=mesh, in_specs=in_specs, out_specs=out_specs, check_vma=False)
```

```python
import functools

import jax
import jax.numpy as jnp
from jax import lax
from jax.experimental import pallas as pl
from jax.experimental.pallas import tpu as pltpu
from jax.sharding import PartitionSpec as P


EPS = 1e-06
VMEM_BYTES = 16 * 2**20


def dot(a, b, dims=((1,), (0,))):
    return lax.dot_general(a, b, (dims, ((), ())), preferred_element_type=jnp.float32)


def lane_sum(a):
    return jnp.sum(a, axis=-1, keepdims=True)


def split(a):
    high = a.astype(jnp.bfloat16)
    return high, (a - high.astype(jnp.float32)).astype(jnp.bfloat16)


def partner(index, shift, size):
    return index ^ shift if size & (size - 1) == 0 else (index + shift) % size


def source(index, shift, size):
    return index ^ shift if size & (size - 1) == 0 else (index - shift) % size


def shift_order(size):
    return [*range(size // 2, size), *range(1, size // 2)]


def exchange(arrays, size):
    got = {}
    for s in shift_order(size):
        got[s] = lax.ppermute(arrays[s], "head", [(i, partner(i, s, size)) for i in range(size)])
    return [got[s] for s in range(1, size)]


def call(kernel, out_shape, scratch=()):
    return pl.pallas_call(
        kernel,
        out_shape=out_shape,
        scratch_shapes=[pltpu.VMEM(shape, dtype) for shape, dtype in scratch],
        compiler_params=pltpu.CompilerParams(vmem_limit_bytes=VMEM_BYTES),
    )


def pack_kernel(gram_ref, memory_ref, gram_out, memory_out):
    pairs, width, _ = gram_out.shape
    size = width // 2
    for p in range(pairs):
        for i in range(2):
            high, low = split(gram_ref[2 * p + i])
            gram_out[p, :size, i * size : (i + 1) * size] = high
            gram_out[p, size:, i * size : (i + 1) * size] = low
            high, low = split(memory_ref[2 * p + i])
            memory_out[p, i * size : (i + 1) * size, :size] = high
            memory_out[p, i * size : (i + 1) * size, size:] = low


def slice_kernel(shards, weight_ref, own_ref, *piece_refs):
    me = lax.axis_index("head")
    half, cols = piece_refs[0].shape
    mine = pl.multiple_of((lax.axis_index("batch") % 2) * half, half)
    own_ref[...] = weight_ref[:, pl.ds(pl.multiple_of(me * cols, cols), cols)]
    for s in range(1, shards):
        off = pl.multiple_of(partner(me, s, shards) * cols, cols)
        piece_refs[s - 1][...] = weight_ref[pl.ds(mine, half), pl.ds(off, cols)]


def join_kernel(*refs):
    half = refs[0].shape[0]
    for s, ref in enumerate(refs[:-1]):
        refs[-1][s * half : (s + 1) * half] = ref[...]


def mesa_kernel(shards, steps, *refs):
    x_refs = refs[:shards]
    w_ref, gate_ref, bias_ref, gain_ref, gram_ref, memory_ref, out_ref, wire_ref, kq, ab, xs, ys = refs[shards:]
    rows, features = x_refs[0].shape
    seqs = rows // steps
    size = out_ref.shape[1]
    me = lax.axis_index("head")
    projected = 0.0
    gate = 0.0
    for s in range(shards):
        off = pl.multiple_of(source(me, s, shards) * features, features)
        projected = projected + dot(x_refs[s][...], w_ref[pl.ds(off, features), :])
        gate_rows = jnp.broadcast_to(gate_ref[:, pl.ds(off, features)], (size, features))
        gate = gate + dot(x_refs[s][...], gate_rows, ((1,), (1,)))
    forget = 0.8 + 0.2 * jax.nn.sigmoid(gate + bias_ref[...])
    queries = projected[:, :size]
    keys = projected[:, size : 2 * size]
    values = projected[:, 2 * size :]
    keys = keys * lax.rsqrt(lane_sum(keys * keys) + EPS)
    queries = queries * lax.rsqrt(lane_sum(queries * queries) + EPS)
    kq[:rows] = keys
    kq[rows:] = queries
    for p in range(seqs // 2):
        parts = []
        for i in range(2):
            parts += split(kq[pl.ds(2 * p + i, 2 * steps, stride=seqs), :])
        lhs = jnp.concatenate(parts, axis=0)
        res = dot(jnp.concatenate([lhs, lhs], axis=1), gram_ref[p])
        for i in range(2):
            half = res[i * 4 * steps : (i + 1) * 4 * steps, i * size : (i + 1) * size]
            ab[pl.ds(2 * p + i, 2 * steps, stride=seqs), :] = half[: 2 * steps] + half[2 * steps :]

    def at(array, t):
        return array[t * seqs : (t + 1) * seqs]

    k = [at(keys, t) for t in range(steps)]
    q = [at(queries, t) for t in range(steps)]
    a = [ab[t * seqs : (t + 1) * seqs, :] for t in range(steps)]
    b = [ab[rows + t * seqs : rows + (t + 1) * seqs, :] for t in range(steps)]
    decay = []
    for t in range(steps):
        decay.append(at(forget, t) if t == 0 else decay[-1] * at(forget, t))
    for s in range(steps):
        g = a[s]
        u = g / (decay[s] + lane_sum(g * k[s]))
        for t in range(s + 1, steps):
            a[t] = a[t] - u * lane_sum(g * k[t])
        for t in range(s, steps):
            b[t] = b[t] - u * lane_sum(g * q[t])
    for t in range(steps):
        xs[t * seqs : (t + 1) * seqs, :] = b[t]
    for p in range(seqs // 2):
        parts = []
        for i in range(2):
            parts += split(xs[pl.ds(2 * p + i, steps, stride=seqs), :])
        lhs = jnp.concatenate(parts, axis=0)
        res = dot(jnp.concatenate([lhs, lhs], axis=1), memory_ref[p], ((1,), (1,)))
        for i in range(2):
            half = res[i * 2 * steps : (i + 1) * 2 * steps, i * size : (i + 1) * size]
            ys[pl.ds(2 * p + i, steps, stride=seqs), :] = half[:steps] + half[steps:]
    scaled = [at(values, t) / decay[t] for t in range(steps)]
    for t in range(steps):
        y = ys[t * seqs : (t + 1) * seqs, :]
        for s in range(t + 1):
            y = y + scaled[s] * lane_sum(k[s] * b[t])
        ys[t * seqs : (t + 1) * seqs, :] = y
    readout = ys[...]
    gained = gain_ref[...] * readout
    out_ref[...] = gained
    wire_ref[:rows] = gained.astype(jnp.bfloat16)
    ones = jnp.ones((wire_ref.shape[0] - rows, size), jnp.bfloat16)
    high, low = split(readout * readout)
    high, low = split(dot(ones, high, ((1,), (1,))) + dot(ones, low, ((1,), (1,))))
    row = lax.broadcasted_iota(jnp.int32, high.shape, 0)
    terms = jnp.where(row == 0, high.astype(jnp.float32), jnp.where(row == 1, low.astype(jnp.float32), 0.0))
    wire_ref[rows:] = terms.astype(jnp.bfloat16)


def output_kernel(shards, *refs):
    wire_refs = refs[:shards]
    own_ref, w_own_ref, mine_ref, other_ref, out_ref, w_scr = refs[shards:]
    rows, size = own_ref.shape
    half = mine_ref.shape[0] // (shards - 1)
    mine = pl.multiple_of((lax.axis_index("batch") % 2) * half, half)
    other = pl.multiple_of(half - mine, half)
    for s in range(1, shards):
        w_scr[pl.ds((s - 1) * size + mine, half), :] = mine_ref[(s - 1) * half : s * half]
        w_scr[pl.ds((s - 1) * size + other, half), :] = other_ref[(s - 1) * half : s * half]
    terms = jnp.concatenate([ref[rows:] for ref in wire_refs], axis=0)
    total = dot(terms, jnp.ones((terms.shape[0], size), jnp.bfloat16), ((0,), (0,)))
    scale = lax.rsqrt(total / (size * shards) + EPS)
    theirs = dot(jnp.concatenate([ref[:rows] for ref in wire_refs[1:]], axis=1), w_scr[...])
    ours = dot((own_ref[...] * scale).astype(jnp.bfloat16), w_own_ref[...])
    out_ref[...] = ours + theirs * jnp.concatenate([scale] * (out_ref.shape[1] // size), axis=1)


def local(inputs, in_weight, gate_weight, gate_bias, norm_gain, out_weight, inv_gram, value_key):
    steps, seqs, features = inputs.shape
    d_model, local_heads, width = in_weight.shape
    assert local_heads == 1 and seqs % 2 == 0 and lax.axis_size("batch") % 2 == 0
    size = width // 3
    rows = steps * seqs
    shards = lax.axis_size("head")
    out_cols = out_weight.shape[1] // shards
    x = inputs.reshape(rows, features)
    groups = lax.axis_size("batch")
    half = size // 2
    xs = [x] + exchange([x] * shards, shards)
    piece = jax.ShapeDtypeStruct((half, out_cols), jnp.bfloat16)
    w_own, *ws = call(
        functools.partial(slice_kernel, shards),
        [jax.ShapeDtypeStruct((size, out_cols), jnp.bfloat16)] + [piece] * (shards - 1),
    )(out_weight)
    ws = exchange([None, *ws], shards)
    weight = in_weight.reshape(d_model, width)
    tiles = jax.ShapeDtypeStruct((seqs // 2, 2 * size, 2 * size), jnp.bfloat16)
    gram, memory = call(pack_kernel, (tiles, tiles))(
        inv_gram.reshape(seqs, size, size), value_key.reshape(seqs, size, size)
    )
    readout, wire = call(
        functools.partial(mesa_kernel, shards, steps),
        (
            jax.ShapeDtypeStruct((rows, size), jnp.float32),
            jax.ShapeDtypeStruct((rows + 16, size), jnp.bfloat16),
        ),
        [((2 * rows, size), jnp.float32)] * 2 + [((rows, size), jnp.float32)] * 2,
    )(*xs, weight, gate_weight.reshape(1, d_model), gate_bias.reshape(1, 1), norm_gain.reshape(1, size), gram, memory)
    rs = [wire] + exchange([wire] * shards, shards)
    w_mine = call(join_kernel, jax.ShapeDtypeStruct(((shards - 1) * half, out_cols), jnp.bfloat16))(*ws)
    w_other = lax.ppermute(w_mine, "batch", [(i, i ^ 1) for i in range(groups)])
    out = call(
        functools.partial(output_kernel, shards),
        jax.ShapeDtypeStruct((rows, out_cols), jnp.float32),
        [(((shards - 1) * size, out_cols), jnp.bfloat16)],
    )(*rs, readout, w_own, w_mine, w_other)
    return out.reshape(steps, seqs, out_cols)


def solution(mesh):
    in_specs = (
        P(None, "batch", "head"),
        P(None, "head", None),
        P(None, "head"),
        P("head"),
        P("head"),
        P("head", None),
        P("batch", "head", None, None),
        P("batch", "head", None, None),
    )
    out_specs = P(None, "batch", "head")
    return jax.shard_map(local, mesh=mesh, in_specs=in_specs, out_specs=out_specs, check_vma=False)
```
